256 devices in a mesh: parts: 4 (over x, y), owner: 64 (over z, core).
Axes of the slice: x: 2, y: 2, z: 32, core: 2. Of those that a mesh axis runs over, the one named last changes fastest.
The devices are a block of a 4x8x32 slice.
Arguments:
- embeddings: bfloat16 [262144, 768], P(('parts', 'owner')), parts along dimension 0, may hold values from -6 to 6
- cluster_ids: int32 [262144], P(('parts', 'owner')), parts along dimension 0, may hold values from 0 to 255, as said below
- owner_map: int32 [1024], P('parts'), parts along dimension 0, may hold values from 0 to 63, as said below
Outputs:
- maxima: float32 [262144], P(('parts', 'owner')), parts along dimension 0
- cluster_mean: float32 [1024], P('parts'), parts along dimension 0
The draws below stay inside these ranges and needn't reach their ends.
There are 4 independent parts, one for each index of `parts`. The reference program is written for one: setup_inputs(seed, part) draws one part's arguments, and reference() takes and returns one part's arrays. A program takes and returns all parts, laid end to end along the dimension named above; each array names one. Nothing has to cross between parts.
Inputs may be any that keep to these rules, and one draw needn't show every extreme that they name: `cluster_ids`: cluster of each item. Owners 2k and 2k+1 form a pair; exactly 32 of the items of one device belong to clusters of one pair, so at most 32 to one owner, and in every draw some owner receives exactly 32 items from every device. `owner_map`: every owner owns exactly 4 clusters.
All inputs are finite; a program needn't handle non-finite values.
Results may differ from the reference program's by a relative error of at most 0.0015.
Values may be sent and summed in bfloat16 or wider, within the bound.
A program may use at most 64 MiB of HBM per device.

```python
import jax
import jax.numpy as jnp
from jax import lax

D = 768
ITEMS_DEV = 1024
CL_DEV = 4
CAP = 32
ITEMS = 65536
CLUSTERS = 256
N_OWNER = 64


def route_tables(key):
    base = jax.random.fold_in(key, 7)
    key_perm, key_thresh, key_hot, key_flip, key_items = jax.random.split(base, 5)
    perm = jax.random.permutation(key_perm, CLUSTERS).astype(jnp.int32)
    owner_map = (perm // CL_DEV).astype(jnp.int32)
    inverse = jnp.argsort(perm).astype(jnp.int32)
    cluster_list = inverse.reshape(N_OWNER, CL_DEV)
    pair_count = N_OWNER // 2
    thresh = jax.random.randint(key_thresh, (pair_count,), 1, 8, dtype=jnp.int32)
    hottest = jax.random.randint(key_hot, (), 0, pair_count, dtype=jnp.int32)
    thresh = jnp.where(jnp.arange(pair_count, dtype=jnp.int32) == hottest, 8, thresh)
    flip = jax.random.randint(key_flip, (pair_count,), 0, 2, dtype=jnp.int32)

    def one_source(source_key):
        key_order, key_side, key_left, key_right = jax.random.split(source_key, 4)
        pair_of = jax.random.permutation(key_order, jnp.arange(ITEMS_DEV, dtype=jnp.int32) // CAP)
        side = (jax.random.randint(key_side, (ITEMS_DEV,), 0, 8, dtype=jnp.int32) < thresh[pair_of]).astype(jnp.int32)
        chosen = 2 * pair_of + jnp.abs(side - flip[pair_of])
        left = jax.random.randint(key_left, (ITEMS_DEV,), 0, CL_DEV, dtype=jnp.int32)
        right = jax.random.randint(key_right, (ITEMS_DEV,), 0, CL_DEV, dtype=jnp.int32)
        return cluster_list[chosen, jnp.minimum(left, right)]
    cluster_ids = jax.vmap(one_source)(jax.random.split(key_items, N_OWNER)).reshape(-1).astype(jnp.int32)
    return (owner_map, cluster_ids)


def draw_cluster_ids(key, part):
    return route_tables(key)[1]


def draw_owner_map(key, part):
    return route_tables(key)[0]


def steps_of(rng, shape, shards, low, high):
    factor_of, own = 1.0, jax.random.fold_in(rng, 6)
    for dim, shards_of in shards:
        steps = jnp.exp(jax.random.uniform(jax.random.fold_in(own, dim), (shards_of,), jnp.float32, low / len(shards), high / len(shards)))
        factor_of = factor_of * jnp.repeat(steps, shape[dim] // shards_of).reshape([-1 if axis == dim else 1 for axis in range(len(shape))])
    return factor_of


def normal_values(rng, shape, deviation, reach, pieces=(), held_as=jnp.bfloat16):
    gain = steps_of(rng, shape, pieces, -0.22, 0.18) if pieces else 1.0
    entries = jax.random.normal(rng, shape, jnp.float32) * deviation * gain
    return jnp.minimum(jnp.maximum(entries, -reach), reach).astype(held_as)


def setup_inputs(seed: int = 0, part: int = 0) -> dict:
    seeds = jax.random.split(jax.random.key(seed), 4)
    part_keys = jax.random.split(jax.random.fold_in(seeds[3], part), 4)
    embeddings = normal_values(part_keys[0], (ITEMS, D), 1.0, 6.0, ((0, 64),))
    cluster_ids = draw_cluster_ids(jax.random.fold_in(jax.random.fold_in(seeds[3], part), 71), part)
    owner_map = draw_owner_map(jax.random.fold_in(jax.random.fold_in(seeds[3], part), 71), part)
    return dict(embeddings=embeddings, cluster_ids=cluster_ids, owner_map=owner_map)


def unitize(rows):
    values = rows.astype(jnp.float32)
    scale = lax.rsqrt(lax.optimization_barrier(jnp.mean(values * values, axis=-1, keepdims=True)) + 1e-06)
    return (values * scale / jnp.sqrt(jnp.float32(D))).astype(jnp.bfloat16)

def reference(embeddings, cluster_ids, owner_map):
    total_items = ITEMS_DEV * N_OWNER
    received = N_OWNER * CAP
    unit = unitize(embeddings).astype(jnp.float32)
    owner_of = owner_map[cluster_ids]
    positions = jnp.arange(received, dtype=jnp.int32)
    distinct = positions[:, None] != positions[None, :]

    def per_owner(carry, owner):
        order = jnp.argsort((owner_of != owner).astype(jnp.int32), stable=True)[:received].astype(jnp.int32)
        valid = owner_of[order] == owner
        labels = jnp.where(valid, cluster_ids[order], -1)
        rows = unit[order]
        gram = jnp.dot(rows, rows.T, precision=lax.Precision.HIGHEST, preferred_element_type=jnp.float32)
        mask = (labels[:, None] == labels[None, :]) & (labels[:, None] >= 0) & distinct
        best = lax.optimization_barrier(jnp.max(jnp.where(mask, gram, jnp.float32(-1.0)), axis=1))
        target = jnp.where(valid, order, total_items).astype(jnp.int32)
        return (carry.at[target].set(best, mode='drop'), None)
    start = jnp.full((total_items,), -1.0, jnp.float32)
    maxima, _ = lax.scan(per_owner, start, jnp.arange(N_OWNER, dtype=jnp.int32))
    totals = jax.ops.segment_sum(maxima, cluster_ids, num_segments=CLUSTERS)
    counts = jax.ops.segment_sum(jnp.ones_like(maxima), cluster_ids, num_segments=CLUSTERS)
    return (maxima, totals / jnp.maximum(counts, 1.0))
```

```python
import functools
import math

import jax
import jax.numpy as jnp
from jax import lax
from jax.experimental import pallas as pl
from jax.experimental.pallas import tpu as pltpu
from jax.sharding import PartitionSpec as P

MESH = pl.DeviceIdType.MESH
LANES = 128
GROUPS = ((0, 16), (16, 24), (24, 28), (28, 32))
NT = (((1,), (1,)), ((), ()))
TN = (((0,), (0,)), ((), ()))


def iota(shape, dim):
    return lax.broadcasted_iota(jnp.int32, shape, dim)


def upto(n):
    return jnp.where(iota((n, n), 0) <= iota((n, n), 1), 1.0, 0.0).astype(jnp.bfloat16)


def product(a, b, dims=(((1,), (0,)), ((), ()))):
    return lax.dot_general(a, b, dims, preferred_element_type=jnp.float32)


def delta_of(pos, chips):
    if pos == 0:
        return 0
    return (chips + 1 - pos) // 2 if pos % 2 else (pos + chips) // 2


def place_of(delta, chips):
    ahead = jnp.where(delta <= chips // 2, chips + 1 - 2 * delta, 2 * delta - chips)
    return jnp.where(delta == 0, 0, ahead)


def three_parts(x):
    high = x.astype(jnp.bfloat16)
    rest = x - high.astype(jnp.float32)
    middle = rest.astype(jnp.bfloat16)
    low = (rest - middle.astype(jnp.float32)).astype(jnp.bfloat16)
    return high, middle, low


def kernel(
    chips, ids_ref, map_ref, rows_ref, max_ref, mean_ref,
    send, keys, lab_s, lab_r, lab_q, lab_k, acc, ret_s, ret_r, mp_s, mp_r, place, lane_at,
    data_ss, data_rs, lab_ss, lab_rs, fwd_ss, fwd_rs, ret_ss, ret_rs, two_ss, two_rs,
):
    items, width = rows_ref.shape
    clusters = map_ref.shape[1]
    block = items // chips
    per = LANES // block
    me = lax.axis_index("owner")
    core, z = lax.rem(me, 2), me // 2
    partner = {"owner": z * 2 + 1 - core}

    def chip(delta):
        return {"owner": lax.rem(z + delta + 2 * chips, chips) * 2 + core}

    barrier = pltpu.get_barrier_semaphore()
    for pos in range(1, chips):
        pl.semaphore_signal(barrier, inc=1, device_id=chip(delta_of(pos, chips)), device_id_type=MESH)
    pl.semaphore_signal(barrier, inc=1, device_id=partner, device_id_type=MESH)

    pair_c = lax.shift_right_logical(map_ref[...], 1)
    place_c = place_of(lax.rem(pair_c - z + chips, chips), chips)
    at_c = jnp.where(iota((chips, clusters), 0) == place_c, 1.0, 0.0)
    count_c = product(at_c.astype(jnp.bfloat16), upto(clusters))
    local_c = jnp.sum(at_c * count_c, axis=0, keepdims=True) - 1.0

    hits = jnp.where(iota((clusters, items), 0) == ids_ref[...], 1.0, 0.0).astype(jnp.bfloat16)
    table = jnp.concatenate([at_c, jnp.broadcast_to(local_c, (16, clusters))], axis=0).astype(jnp.bfloat16)
    found = product(table, hits)
    at = found[:chips]
    label = found[chips:].astype(jnp.bfloat16)
    tiles = items // LANES
    stacked = jnp.concatenate([at[:, t * LANES : (t + 1) * LANES] for t in range(tiles)], axis=0)
    sums = product(stacked.astype(jnp.bfloat16), upto(LANES))
    row = iota((chips, LANES), 0).astype(jnp.float32)
    before = jnp.zeros((chips, 1), jnp.float32)
    places, slots = [], []
    for t in range(tiles):
        at_t = stacked[t * chips : (t + 1) * chips]
        sum_t = sums[t * chips : (t + 1) * chips]
        places.append(jnp.sum(at_t * row, axis=0, keepdims=True))
        slots.append(jnp.sum(at_t * (sum_t + before + row * block), axis=0, keepdims=True) - 1.0)
        before = before + sum_t[:, LANES - 1 :]
    place_i = jnp.concatenate(places, axis=1).astype(jnp.int32)
    slot = jnp.concatenate(slots, axis=1).astype(jnp.int32)
    place[:, :items] = place_i
    place[:, items:] = place_c
    lane_at[:, :items] = lax.rem(slot, LANES)
    lane_at[:, items:] = lax.rem(place_c + 1, per) * block + local_c.astype(jnp.int32)

    def data_copy(pos):
        return pltpu.make_async_remote_copy(
            src_ref=send.at[pl.ds(pos * block, block)], dst_ref=keys.at[pl.ds(pos * block, block)],
            send_sem=data_ss.at[pos], recv_sem=data_rs.at[pos],
            device_id=chip(delta_of(pos, chips)), device_id_type=MESH,
        )

    def label_copy(pos):
        return pltpu.make_async_remote_copy(
            src_ref=lab_s.at[pos // per], dst_ref=lab_r.at[pos],
            send_sem=lab_ss.at[pos], recv_sem=lab_rs.at[pos],
            device_id=chip(delta_of(pos, chips)), device_id_type=MESH,
        )

    def forward_copy(pos):
        return pltpu.make_async_remote_copy(
            src_ref=keys.at[pl.ds(pos * block, block)], dst_ref=keys.at[pl.ds(items + pos * block, block)],
            send_sem=fwd_ss.at[pos], recv_sem=fwd_rs.at[pos], device_id=partner, device_id_type=MESH,
        )

    def return_copy(pos):
        return pltpu.make_async_remote_copy(
            src_ref=ret_s.at[pos], dst_ref=ret_r.at[pos],
            send_sem=ret_ss.at[pos], recv_sem=ret_rs.at[pos],
            device_id=chip(-delta_of(pos, chips)), device_id_type=MESH,
        )

    labels_over = pltpu.make_async_remote_copy(
        src_ref=lab_r.at[pl.ds(0, chips)], dst_ref=lab_r.at[pl.ds(chips, chips)],
        send_sem=two_ss.at[0], recv_sem=two_rs.at[0], device_id=partner, device_id_type=MESH,
    )
    means_over = pltpu.make_async_remote_copy(
        src_ref=mp_s, dst_ref=mp_r,
        send_sem=two_ss.at[1], recv_sem=two_rs.at[1], device_id=partner, device_id_type=MESH,
    )

    step = 2 * LANES
    for first in range(0, items, step):
        pick = jnp.where(iota((step, items), 0) + first == slot, 1.0, 0.0).astype(jnp.bfloat16)
        rows = product(pick, rows_ref[...])
        scale = lax.rsqrt(jnp.mean(rows * rows, axis=1, keepdims=True) + 1e-06)
        unit = (rows * scale * jnp.float32(width**-0.5)).astype(jnp.bfloat16)
        send[first : first + step] = unit
        names = product(label, pick, NT)
        for t in range(step // LANES):
            lab_s[first // LANES + t] = names[:1, t * LANES : (t + 1) * LANES]
        if first == 0:
            keys[:block] = unit[:block]
            lab_r[0] = names[:1, :LANES]
            pl.semaphore_wait(barrier, chips)
        for pos in range(first // block, (first + step) // block):
            if pos > 0:
                data_copy(pos).start()
                label_copy(pos).start()
    forward_copy(0).start()

    for pos in range(1, chips):
        label_copy(pos).wait_recv()
    labels_over.start()
    labels_over.wait_recv()
    quarter = lax.div(iota((1, LANES), 1), block)
    for t in range(2 * tiles):
        mixed = jnp.zeros((1, LANES), jnp.float32)
        for q in range(per):
            mixed = jnp.where(quarter == q, lab_r[t * per + q], mixed)
        lab_q[:, t * LANES : (t + 1) * LANES] = mixed
        lab_k[t * LANES : (t + 1) * LANES] = jnp.broadcast_to(mixed, (LANES, LANES)).T
    acc[...] = jnp.full(acc.shape, -1.0, jnp.float32)

    def meet(k0, kn, q0, qn, own):
        gram = product(keys[pl.ds(k0, kn)], keys[q0 : q0 + qn], NT)
        same = jnp.concatenate([lab_k[pl.ds(k0, kn)]] * (qn // LANES), axis=1) == lab_q[:, q0 : q0 + qn]
        if own:
            same = same & (iota((kn, qn), 0) + k0 != iota((kn, qn), 1) + q0)
        best = jnp.where(same, gram, -1.0)
        acc[:, q0 : q0 + qn] = jnp.maximum(acc[:, q0 : q0 + qn], jnp.max(best.reshape(kn // 8, 8, qn), axis=0))

    def meet_all(k0, kn, q0, qn, own):
        size = math.gcd(kn, 2 * LANES)
        if kn == size:
            meet(k0, kn, q0, qn, own)
        else:
            @pl.loop(0, kn // size)
            def _(i):
                meet(pl.multiple_of(k0 + i * size, LANES), size, q0, qn, own)

    for low, high in GROUPS:
        for pos in range(low, high):
            if pos > 0:
                data_copy(pos).wait_recv()
                forward_copy(pos).start()
        for pos in range(low, high):
            forward_copy(pos).wait_recv()
        old, new, end = low * block, (high - low) * block, high * block
        meet_all(old, new, 0, end, True)
        meet_all(items + old, new, 0, end, False)
        if old:
            meet_all(0, old, old, new, False)
            meet_all(items, old, old, new, False)

    best = jnp.max(acc[...], axis=0, keepdims=True)
    kinds = 8
    kind = iota((kinds, items), 0).astype(jnp.float32)
    mine = jnp.where(kind == lab_q[:, :items], 1.0, 0.0)
    other = jnp.where(kind == lab_q[:, items:], 1.0, 0.0)
    numbers = jnp.sum(mine + other, axis=1, keepdims=True)
    part = jnp.sum(mine * best, axis=1, keepdims=True) / jnp.maximum(numbers, 1.0)
    spread = jnp.where(iota((kinds, LANES), 0) == lax.rem(iota((kinds, LANES), 1), kinds), part, 0.0)
    parts = jnp.sum(spread, axis=0, keepdims=True)
    for pos in range(chips):
        first = pos // per * LANES
        packed = jnp.where(quarter == pos % per, best[:, first : first + LANES], parts)
        if pos == 0:
            ret_r[0] = packed
        else:
            ret_s[pos] = packed
    for pos in range(1, chips):
        return_copy(pos).start()

    for pos in range(chips):
        if pos > 0:
            data_copy(pos).wait_send()
            label_copy(pos).wait_send()
        forward_copy(pos).wait_send()
    labels_over.wait_send()
    total = items + clusters
    here = jnp.where(iota((chips, total), 0) == place[...], 1.0, 0.0).astype(jnp.bfloat16)
    here = jnp.concatenate([here] * 3, axis=0)
    wanted = iota((LANES, total), 0) == lane_at[...]
    for pos in range(1, chips):
        return_copy(pos).wait_recv()
    back = jnp.concatenate([ret_r[pos] for pos in range(chips)], axis=0)
    values = product(jnp.concatenate(three_parts(back), axis=0), here, TN)
    out = jnp.sum(jnp.where(wanted, values, 0.0), axis=0, keepdims=True)
    mp_s[...] = out[:, items:]
    means_over.start()
    max_ref[...] = out[:, :items]
    for pos in range(1, chips):
        return_copy(pos).wait_send()
    means_over.wait()
    mean_ref[...] = mp_s[...] + mp_r[...]


def body(embeddings, cluster_ids, owner_map):
    chips = lax.axis_size("owner") // 2
    items, width = embeddings.shape
    clusters = owner_map.shape[0]
    vmem = pl.BlockSpec(memory_space=pltpu.VMEM)
    row = (1, LANES)
    copies = [pltpu.SemaphoreType.DMA((chips,))] * 2
    maxima, means = pl.pallas_call(
        functools.partial(kernel, chips),
        out_shape=(
            jax.ShapeDtypeStruct((1, items), jnp.float32),
            jax.ShapeDtypeStruct((1, clusters), jnp.float32),
        ),
        in_specs=[vmem] * 3,
        out_specs=(vmem, vmem),
        scratch_shapes=[
            pltpu.VMEM((items, width), jnp.bfloat16),
            pltpu.VMEM((2 * items, width), jnp.bfloat16),
            pltpu.VMEM((items // LANES, *row), jnp.float32),
            pltpu.VMEM((2 * chips, *row), jnp.float32),
            pltpu.VMEM((1, 2 * items), jnp.float32),
            pltpu.VMEM((2 * items, LANES), jnp.float32),
            pltpu.VMEM((8, items), jnp.float32),
            pltpu.VMEM((chips, *row), jnp.float32),
            pltpu.VMEM((chips, *row), jnp.float32),
            pltpu.VMEM((1, clusters), jnp.float32),
            pltpu.VMEM((1, clusters), jnp.float32),
            pltpu.VMEM((1, items + clusters), jnp.int32),
            pltpu.VMEM((1, items + clusters), jnp.int32),
            *copies, *copies, *copies, *copies,
            *[pltpu.SemaphoreType.DMA((2,))] * 2,
        ],
        compiler_params=pltpu.CompilerParams(collective_id=0, has_side_effects=True),
    )(cluster_ids.reshape(1, items), owner_map.reshape(1, clusters), embeddings)
    return maxima.reshape(items), means.reshape(clusters)


def solution(mesh):
    placed = (P(("parts", "owner"), None), P(("parts", "owner")), P("parts"))
    return jax.shard_map(
        body,
        mesh=mesh,
        in_specs=placed,
        out_specs=(P(("parts", "owner")), P("parts")),
        check_vma=False,
    )
```

```python
import functools
import math

import jax
import jax.numpy as jnp
from jax import lax
from jax.experimental import pallas as pl
from jax.experimental.pallas import tpu as pltpu
from jax.sharding import PartitionSpec as P

MESH = pl.DeviceIdType.MESH
LANES = 128
GROUPS = ((0, 16), (16, 24), (24, 28))
NT = (((1,), (1,)), ((), ()))
TN = (((0,), (0,)), ((), ()))


def iota(shape, dim):
    return lax.broadcasted_iota(jnp.int32, shape, dim)


def upto(n):
    return jnp.where(iota((n, n), 0) <= iota((n, n), 1), 1.0, 0.0).astype(jnp.bfloat16)


def product(a, b, dims=(((1,), (0,)), ((), ()))):
    return lax.dot_general(a, b, dims, preferred_element_type=jnp.float32)


def deltas(chips):
    half, near = chips // 2, (2, 3, 4)
    order = [0, *(d * way for d in near for way in (1, -1)), half]
    far = [d for d in range(half - 1, 0, -1) if d not in near]
    return order + [d * way for d in far for way in (1, -1)]


def place_of(ahead, chips):
    place = jnp.zeros_like(ahead)
    for pos, delta in enumerate(deltas(chips)):
        place = jnp.where(ahead == delta % chips, pos, place)
    return place


def three_parts(x):
    high = x.astype(jnp.bfloat16)
    rest = x - high.astype(jnp.float32)
    middle = rest.astype(jnp.bfloat16)
    low = (rest - middle.astype(jnp.float32)).astype(jnp.bfloat16)
    return high, middle, low


def kernel(
    chips, ids_hbm, map_hbm, rows_hbm, max_hbm, mean_hbm,
    ids_ref, map_ref, rows_ref, max_ref, mean_ref, send, keys, lab_s, lab_r, lab_q, lab_k, acc, ret_s, ret_r, mp_s, mp_r, place, lane_at,
    data_ss, data_rs, lab_ss, lab_rs, fwd_ss, fwd_rs, ret_ss, ret_rs, two_ss, two_rs, own_sem, known,
):
    items, width = rows_ref.shape
    clusters = map_ref.shape[1]
    block = items // chips
    per = LANES // block
    me = lax.axis_index("owner")
    core, z = lax.rem(me, 2), me // 2
    partner = {"owner": z * 2 + 1 - core}

    def chip(delta):
        return {"owner": lax.rem(z + delta + 2 * chips, chips) * 2 + core}

    def signal(semaphore, device):
        pl.semaphore_signal(semaphore, inc=1, device_id=device, device_id_type=MESH)

    ahead = deltas(chips)
    barrier = pltpu.get_barrier_semaphore()
    for device in (chip(1), chip(-1), partner):
        signal(barrier, device)
    loads = [
        pltpu.make_async_copy(source, target, own_sem.at[i])
        for i, (source, target) in enumerate(((ids_hbm, ids_ref), (map_hbm, map_ref), (rows_hbm, rows_ref)))
    ]
    for load in loads:
        load.start()

    levels = math.ceil(math.log2(chips // 2))

    def tell(level):
        for way in (1, -1):
            signal(known.at[level], chip(way * 2**level))

    def learn(level):
        pl.semaphore_wait(known.at[level], 2)

    loads[0].wait()
    loads[1].wait()

    pair_c = lax.shift_right_logical(map_ref[...], 1)
    place_c = place_of(lax.rem(pair_c - z + chips, chips), chips)
    at_c = jnp.where(iota((chips, clusters), 0) == place_c, 1.0, 0.0)
    count_c = product(at_c.astype(jnp.bfloat16), upto(clusters))
    local_c = jnp.sum(at_c * count_c, axis=0, keepdims=True) - 1.0

    hits = jnp.where(iota((clusters, items), 0) == ids_ref[...], 1.0, 0.0).astype(jnp.bfloat16)
    table = jnp.concatenate([at_c, jnp.broadcast_to(local_c, (16, clusters))], axis=0).astype(jnp.bfloat16)
    found = product(table, hits)
    at = found[:chips]
    label = found[chips:].astype(jnp.bfloat16)
    tiles = items // LANES
    stacked = jnp.concatenate([at[:, t * LANES : (t + 1) * LANES] for t in range(tiles)], axis=0)
    sums = product(stacked.astype(jnp.bfloat16), upto(LANES))
    row = iota((chips, LANES), 0).astype(jnp.float32)
    before = jnp.zeros((chips, 1), jnp.float32)
    places, slots = [], []
    for t in range(tiles):
        at_t = stacked[t * chips : (t + 1) * chips]
        sum_t = sums[t * chips : (t + 1) * chips]
        places.append(jnp.sum(at_t * row, axis=0, keepdims=True))
        slots.append(jnp.sum(at_t * (sum_t + before + row * block), axis=0, keepdims=True) - 1.0)
        before = before + sum_t[:, LANES - 1 :]
    place_i = jnp.concatenate(places, axis=1).astype(jnp.int32)
    slot = jnp.concatenate(slots, axis=1).astype(jnp.int32)
    place[:, :items] = place_i
    place[:, items:] = place_c
    lane_at[:, :items] = lax.rem(slot, LANES)
    lane_at[:, items:] = lax.rem(place_c + 1, per) * block + local_c.astype(jnp.int32)

    def data_copy(pos):
        return pltpu.make_async_remote_copy(
            src_ref=send.at[pl.ds(pos * block, block)], dst_ref=keys.at[pl.ds(pos * block, block)],
            send_sem=data_ss.at[pos], recv_sem=data_rs.at[pos],
            device_id=chip(ahead[pos]), device_id_type=MESH,
        )

    def label_copy(pos):
        return pltpu.make_async_remote_copy(
            src_ref=lab_s.at[pos // per], dst_ref=lab_r.at[pos],
            send_sem=lab_ss.at[pos], recv_sem=lab_rs.at[pos],
            device_id=chip(ahead[pos]), device_id_type=MESH,
        )

    def forward_copy(pos):
        return pltpu.make_async_remote_copy(
            src_ref=keys.at[pl.ds(pos * block, block)], dst_ref=keys.at[pl.ds(items + pos * block, block)],
            send_sem=fwd_ss.at[pos], recv_sem=fwd_rs.at[pos], device_id=partner, device_id_type=MESH,
        )

    def return_copy(pos):
        return pltpu.make_async_remote_copy(
            src_ref=ret_s.at[pos], dst_ref=ret_r.at[pos],
            send_sem=ret_ss.at[pos], recv_sem=ret_rs.at[pos],
            device_id=chip(-ahead[pos]), device_id_type=MESH,
        )

    labels_over = pltpu.make_async_remote_copy(
        src_ref=lab_r.at[pl.ds(0, chips)], dst_ref=lab_r.at[pl.ds(chips, chips)],
        send_sem=two_ss.at[0], recv_sem=two_rs.at[0], device_id=partner, device_id_type=MESH,
    )
    means_over = pltpu.make_async_remote_copy(
        src_ref=mp_s, dst_ref=mp_r,
        send_sem=two_ss.at[1], recv_sem=two_rs.at[1], device_id=partner, device_id_type=MESH,
    )

    step = 2 * LANES

    def arrange(first):
        pick = jnp.where(iota((step, items), 0) + first == slot, 1.0, 0.0).astype(jnp.bfloat16)
        rows = product(pick, rows_ref[...])
        scale = lax.rsqrt(jnp.mean(rows * rows, axis=1, keepdims=True) + 1e-06)
        unit = (rows * scale * jnp.float32(width**-0.5)).astype(jnp.bfloat16)
        send[first : first + step] = unit
        names = product(label, pick, NT)
        for t in range(step // LANES):
            lab_s[first // LANES + t] = names[:1, t * LANES : (t + 1) * LANES]
        if first == 0:
            keys[:block] = unit[:block]
            lab_r[0] = names[:1, :LANES]

    def start(copy, low, high):
        for pos in range(1, chips):
            if low <= abs(ahead[pos]) <= high:
                copy(pos).start()

    pl.semaphore_wait(barrier, 3)
    tell(0)
    loads[2].wait()
    arrange(0)
    learn(0)
    tell(1)
    start(label_copy, 2, 2)
    start(data_copy, 2, 2)
    arrange(step)
    learn(1)
    tell(2)
    start(label_copy, 3, 4)
    start(data_copy, 3, 4)
    for first in range(2 * step, items, step):
        arrange(first)
    start(label_copy, 1, 1)
    for level in range(2, levels):
        learn(level)
        if level + 1 < levels:
            tell(level + 1)
        start(label_copy, 2**level + 1, 2 ** (level + 1))
    start(data_copy, 5, chips)
    start(data_copy, 1, 1)
    forward_copy(0).start()

    for pos in range(1, chips):
        label_copy(pos).wait_recv()
    labels_over.start()
    labels_over.wait_recv()
    quarter = lax.div(iota((1, LANES), 1), block)
    for t in range(2 * tiles):
        mixed = jnp.zeros((1, LANES), jnp.float32)
        for q in range(per):
            mixed = jnp.where(quarter == q, lab_r[t * per + q], mixed)
        lab_q[:, t * LANES : (t + 1) * LANES] = mixed
        lab_k[t * LANES : (t + 1) * LANES] = jnp.broadcast_to(mixed, (LANES, LANES)).T
    acc[...] = jnp.full(acc.shape, -1.0, jnp.float32)

    def best_of(gram, k0, q0, own):
        kn, qn = gram.shape
        same = jnp.concatenate([lab_k[pl.ds(k0, kn)]] * (qn // LANES), axis=1) == lab_q[:, q0 : q0 + qn]
        if own:
            same = same & (iota((kn, qn), 0) + k0 != iota((kn, qn), 1) + q0)
        return jnp.where(same, gram, -1.0)

    def meet(k0, kn, q0, qn, own):
        best = best_of(product(keys[pl.ds(k0, kn)], keys[q0 : q0 + qn], NT), k0, q0, own)
        acc[:, q0 : q0 + qn] = jnp.maximum(acc[:, q0 : q0 + qn], jnp.max(best.reshape(kn // 8, 8, qn), axis=0))
        return best

    def meet_all(k0, kn, q0, qn, own):
        size = math.gcd(kn, 2 * LANES)

        @pl.loop(0, kn // size)
        def _(i):
            meet(pl.multiple_of(k0 + i * size, LANES), size, q0, qn, own)

    def arrived(low, high):
        for pos in range(low, high):
            if pos > 0:
                data_copy(pos).wait_recv()
                forward_copy(pos).start()

    def forwarded(low, high):
        for pos in range(low, high):
            forward_copy(pos).wait_recv()

    for low, high in GROUPS:
        arrived(low, high)
        forwarded(low, high)
        old, new, end = low * block, (high - low) * block, high * block
        meet_all(old, new, 0, end, True)
        meet_all(items + old, new, 0, end, False)
        if old:
            meet_all(0, old, old, new, False)
            meet_all(items, old, old, new, False)
    last = GROUPS[-1][1]
    old, new = last * block, items - last * block
    arrived(last, chips)
    here = meet(old, new, 0, items, True)
    there = best_of(product(keys[old:items], keys[items : items + old], NT), old, items, False)
    column = jnp.maximum(jnp.max(here, axis=1, keepdims=True), jnp.max(there, axis=1, keepdims=True))
    line = jnp.broadcast_to(column, (new, LANES)).T[:8]
    acc[:, old:] = jnp.maximum(acc[:, old:], line)
    forwarded(last, chips)
    meet(items + old, new, 0, items, False)

    best = jnp.max(acc[...], axis=0, keepdims=True)
    kinds = 8
    kind = iota((kinds, items), 0).astype(jnp.float32)
    mine = jnp.where(kind == lab_q[:, :items], 1.0, 0.0)
    other = jnp.where(kind == lab_q[:, items:], 1.0, 0.0)
    numbers = jnp.sum(mine + other, axis=1, keepdims=True)
    part = jnp.sum(mine * best, axis=1, keepdims=True) / jnp.maximum(numbers, 1.0)
    spread = jnp.where(iota((kinds, LANES), 0) == lax.rem(iota((kinds, LANES), 1), kinds), part, 0.0)
    parts = jnp.sum(spread, axis=0, keepdims=True)
    for pos in range(chips):
        first = pos // per * LANES
        packed = jnp.where(quarter == pos % per, best[:, first : first + LANES], parts)
        if pos == 0:
            ret_r[0] = packed
        else:
            ret_s[pos] = packed
    for pos in sorted(range(1, chips), key=lambda pos: -abs(ahead[pos])):
        return_copy(pos).start()

    for pos in range(chips):
        if pos > 0:
            data_copy(pos).wait_send()
            label_copy(pos).wait_send()
        forward_copy(pos).wait_send()
    labels_over.wait_send()
    total = items + clusters
    here = jnp.where(iota((chips, total), 0) == place[...], 1.0, 0.0).astype(jnp.bfloat16)
    here = jnp.concatenate([here] * 3, axis=0)
    wanted = iota((LANES, total), 0) == lane_at[...]
    for pos in range(1, chips):
        return_copy(pos).wait_recv()
    back = jnp.concatenate([ret_r[pos] for pos in range(chips)], axis=0)
    back = jnp.concatenate(three_parts(back), axis=0)

    def looked_up(low, high):
        values = product(back, here[:, low:high], TN)
        return jnp.sum(jnp.where(wanted[:, low:high], values, 0.0), axis=0, keepdims=True)

    mp_s[...] = looked_up(items, total)
    means_over.start()
    max_ref[...] = looked_up(0, items)
    store_max = pltpu.make_async_copy(max_ref, max_hbm, own_sem.at[0])
    store_max.start()
    for pos in range(1, chips):
        return_copy(pos).wait_send()
    means_over.wait()
    mean_ref[...] = mp_s[...] + mp_r[...]
    store_mean = pltpu.make_async_copy(mean_ref, mean_hbm, own_sem.at[1])
    store_mean.start()
    store_max.wait()
    store_mean.wait()


def body(embeddings, cluster_ids, owner_map):
    chips = lax.axis_size("owner") // 2
    items, width = embeddings.shape
    clusters = owner_map.shape[0]
    anywhere = pl.BlockSpec(memory_space=pl.ANY)
    row = (1, LANES)
    copies = [pltpu.SemaphoreType.DMA((chips,))] * 2
    maxima, means = pl.pallas_call(
        functools.partial(kernel, chips),
        out_shape=(
            jax.ShapeDtypeStruct((1, items), jnp.float32),
            jax.ShapeDtypeStruct((1, clusters), jnp.float32),
        ),
        in_specs=[anywhere] * 3,
        out_specs=(anywhere, anywhere),
        scratch_shapes=[
            pltpu.VMEM((1, items), jnp.int32),
            pltpu.VMEM((1, clusters), jnp.int32),
            pltpu.VMEM((items, width), jnp.bfloat16),
            pltpu.VMEM((1, items), jnp.float32),
            pltpu.VMEM((1, clusters), jnp.float32),
            pltpu.VMEM((items, width), jnp.bfloat16),
            pltpu.VMEM((2 * items, width), jnp.bfloat16),
            pltpu.VMEM((items // LANES, *row), jnp.float32),
            pltpu.VMEM((2 * chips, *row), jnp.float32),
            pltpu.VMEM((1, 2 * items), jnp.float32),
            pltpu.VMEM((2 * items, LANES), jnp.float32),
            pltpu.VMEM((8, items), jnp.float32),
            pltpu.VMEM((chips, *row), jnp.float32),
            pltpu.VMEM((chips, *row), jnp.float32),
            pltpu.VMEM((1, clusters), jnp.float32),
            pltpu.VMEM((1, clusters), jnp.float32),
            pltpu.VMEM((1, items + clusters), jnp.int32),
            pltpu.VMEM((1, items + clusters), jnp.int32),
            *copies, *copies, *copies, *copies,
            *[pltpu.SemaphoreType.DMA((2,))] * 2,
            pltpu.SemaphoreType.DMA((3,)),
            pltpu.SemaphoreType.REGULAR((8,)),
        ],
        compiler_params=pltpu.CompilerParams(collective_id=0, has_side_effects=True),
    )(cluster_ids.reshape(1, items), owner_map.reshape(1, clusters), embeddings)
    return maxima.reshape(items), means.reshape(clusters)


def solution(mesh):
    placed = (P(("parts", "owner"), None), P(("parts", "owner")), P("parts"))
    return jax.shard_map(
        body,
        mesh=mesh,
        in_specs=placed,
        out_specs=(P(("parts", "owner")), P("parts")),
        check_vma=False,
    )
```

```python
import functools
import math

import jax
import jax.numpy as jnp
from jax import lax
from jax.experimental import pallas as pl
from jax.experimental.pallas import tpu as pltpu
from jax.sharding import PartitionSpec as P

MESH = pl.DeviceIdType.MESH
LANES = 128
GROUPS = ((0, 16), (16, 24), (24, 28), (28, 32))
LAST = 2
NT = (((1,), (1,)), ((), ()))
TN = (((0,), (0,)), ((), ()))


def iota(shape, dim):
    return lax.broadcasted_iota(jnp.int32, shape, dim)


def upto(n):
    return jnp.where(iota((n, n), 0) <= iota((n, n), 1), 1.0, 0.0).astype(jnp.bfloat16)


def product(a, b, dims=(((1,), (0,)), ((), ()))):
    return lax.dot_general(a, b, dims, preferred_element_type=jnp.float32)


def deltas(chips):
    half, near = chips // 2, (2, 3, 4, 5)
    order = [0, *(d * way for d in near for way in (1, -1)), half]
    far = [d for d in range(half - 1, 0, -1) if d not in near]
    return order + [d * way for d in far for way in (1, -1)]


def place_of(ahead, chips):
    place = jnp.zeros_like(ahead)
    for pos, delta in enumerate(deltas(chips)):
        place = jnp.where(ahead == delta % chips, pos, place)
    return place


def three_parts(x):
    high = x.astype(jnp.bfloat16)
    rest = x - high.astype(jnp.float32)
    middle = rest.astype(jnp.bfloat16)
    low = (rest - middle.astype(jnp.float32)).astype(jnp.bfloat16)
    return high, middle, low


def kernel(
    chips, ids_hbm, map_hbm, rows_hbm, out_hbm,
    ids_ref, map_ref, rows_ref, out_ref, send, keys, lab_s, lab_r, lab_q, lab_k, acc, ret_s, ret_r, par_s, par_r, place, lane_at,
    data_ss, data_rs, lab_ss, lab_rs, fwd_ss, fwd_rs, ret_ss, ret_rs, par_ss, par_rs, two_ss, two_rs, own_sem, known,
):
    items, width = rows_ref.shape
    clusters = map_ref.shape[1]
    block = items // chips
    per = LANES // block
    me = lax.axis_index("owner")
    core, z = lax.rem(me, 2), me // 2
    partner = {"owner": z * 2 + 1 - core}

    def chip(delta, which=core):
        return {"owner": lax.rem(z + delta + 2 * chips, chips) * 2 + which}

    def all_of(ref, semaphore):
        pltpu.make_async_copy(ref, ref, semaphore).wait()

    def signal(semaphore, device):
        pl.semaphore_signal(semaphore, inc=1, device_id=device, device_id_type=MESH)

    ahead = deltas(chips)
    barrier = pltpu.get_barrier_semaphore()
    for device in (chip(1), chip(-1), partner):
        signal(barrier, device)
    loads = [
        pltpu.make_async_copy(source, target, own_sem.at[i])
        for i, (source, target) in enumerate(((ids_hbm, ids_ref), (map_hbm, map_ref), (rows_hbm, rows_ref)))
    ]
    for load in loads:
        load.start()

    levels = math.ceil(math.log2(chips // 2))

    def tell(level):
        for way in (1, -1):
            signal(known.at[level], chip(way * 2**level))

    def learn(level):
        pl.semaphore_wait(known.at[level], 2)

    loads[0].wait()
    loads[1].wait()

    pair_c = lax.shift_right_logical(map_ref[...], 1)
    place_c = place_of(lax.rem(pair_c - z + chips, chips), chips)
    at_c = jnp.where(iota((chips, clusters), 0) == place_c, 1.0, 0.0)
    count_c = product(at_c.astype(jnp.bfloat16), upto(clusters))
    local_c = jnp.sum(at_c * count_c, axis=0, keepdims=True) - 1.0

    hits = jnp.where(iota((clusters, items), 0) == ids_ref[...], 1.0, 0.0).astype(jnp.bfloat16)
    table = jnp.concatenate([at_c, jnp.broadcast_to(local_c, (16, clusters))], axis=0).astype(jnp.bfloat16)
    found = product(table, hits)
    at = found[:chips]
    label = found[chips:].astype(jnp.bfloat16)
    tiles = items // LANES
    stacked = jnp.concatenate([at[:, t * LANES : (t + 1) * LANES] for t in range(tiles)], axis=0)
    sums = product(stacked.astype(jnp.bfloat16), upto(LANES))
    row = iota((chips, LANES), 0).astype(jnp.float32)
    before = jnp.zeros((chips, 1), jnp.float32)
    places, slots = [], []
    for t in range(tiles):
        at_t = stacked[t * chips : (t + 1) * chips]
        sum_t = sums[t * chips : (t + 1) * chips]
        places.append(jnp.sum(at_t * row, axis=0, keepdims=True))
        slots.append(jnp.sum(at_t * (sum_t + before + row * block), axis=0, keepdims=True) - 1.0)
        before = before + sum_t[:, LANES - 1 :]
    place_i = jnp.concatenate(places, axis=1).astype(jnp.int32)
    slot = jnp.concatenate(slots, axis=1).astype(jnp.int32)
    place[:, :items] = place_i
    place[:, items:] = place_c
    lane_at[:, :items] = lax.rem(slot, LANES)
    lane_at[:, items:] = lax.rem(place_c + 1, per) * block + local_c.astype(jnp.int32)

    group_of = {pos: g for g, (low, high) in enumerate(GROUPS) for pos in range(low, high)}

    def data_copy(pos):
        return pltpu.make_async_remote_copy(
            src_ref=send.at[pl.ds(pos * block, block)], dst_ref=keys.at[pl.ds(pos * block, block)],
            send_sem=data_ss, recv_sem=data_rs.at[group_of[pos]],
            device_id=chip(ahead[pos]), device_id_type=MESH,
        )

    def label_copy(pos):
        return pltpu.make_async_remote_copy(
            src_ref=lab_s.at[pos // per], dst_ref=lab_r.at[pos],
            send_sem=lab_ss, recv_sem=lab_rs,
            device_id=chip(ahead[pos]), device_id_type=MESH,
        )

    def forward_copy(g):
        low, high = GROUPS[g]
        return pltpu.make_async_remote_copy(
            src_ref=keys.at[pl.ds(low * block, (high - low) * block)],
            dst_ref=keys.at[pl.ds(items + low * block, (high - low) * block)],
            send_sem=fwd_ss, recv_sem=fwd_rs.at[g], device_id=partner, device_id_type=MESH,
        )

    def return_copy(pos):
        return pltpu.make_async_remote_copy(
            src_ref=ret_s.at[pos], dst_ref=ret_r.at[pos],
            send_sem=ret_ss, recv_sem=ret_rs,
            device_id=chip(-ahead[pos]), device_id_type=MESH,
        )

    def part_copy(pos):
        return pltpu.make_async_remote_copy(
            src_ref=par_s, dst_ref=par_r.at[pos],
            send_sem=par_ss, recv_sem=par_rs,
            device_id=chip(-ahead[pos], 1 - core), device_id_type=MESH,
        )

    labels_over = pltpu.make_async_remote_copy(
        src_ref=lab_r.at[pl.ds(0, chips)], dst_ref=lab_r.at[pl.ds(chips, chips)],
        send_sem=two_ss, recv_sem=two_rs, device_id=partner, device_id_type=MESH,
    )

    step = 2 * LANES

    def arrange(first):
        pick = jnp.where(iota((step, items), 0) + first == slot, 1.0, 0.0).astype(jnp.bfloat16)
        rows = product(pick, rows_ref[...])
        scale = lax.rsqrt(jnp.mean(rows * rows, axis=1, keepdims=True) + 1e-06)
        unit = (rows * scale * jnp.float32(width**-0.5)).astype(jnp.bfloat16)
        send[first : first + step] = unit
        names = product(label, pick, NT)
        for t in range(step // LANES):
            lab_s[first // LANES + t] = names[:1, t * LANES : (t + 1) * LANES]
        if first == 0:
            keys[:block] = unit[:block]
            lab_r[0] = names[:1, :LANES]

    def start(copy, low, high):
        for pos in range(1, chips):
            if low <= abs(ahead[pos]) <= high:
                copy(pos).start()

    pl.semaphore_wait(barrier, 3)
    tell(0)
    loads[2].wait()
    arrange(0)
    arrange(step)
    learn(0)
    tell(1)
    start(label_copy, 2, 2)
    start(data_copy, 2, 2)
    arrange(2 * step)
    learn(1)
    tell(2)
    start(label_copy, 3, 4)
    start(data_copy, 3, 4)
    for first in range(3 * step, items, step):
        arrange(first)
    start(label_copy, 1, 1)
    for level in range(2, levels):
        learn(level)
        if level + 1 < levels:
            tell(level + 1)
        start(label_copy, 2**level + 1, 2 ** (level + 1))
        if level == 2:
            start(data_copy, 5, 5)
    start(data_copy, 6, chips)
    start(data_copy, 1, 1)

    all_of(lab_r.at[pl.ds(1, chips - 1)], lab_rs)
    labels_over.start()
    labels_over.wait_recv()
    quarter = lax.div(iota((1, LANES), 1), block)
    for t in range(2 * tiles):
        mixed = jnp.zeros((1, LANES), jnp.float32)
        for q in range(per):
            mixed = jnp.where(quarter == q, lab_r[t * per + q], mixed)
        lab_q[:, t * LANES : (t + 1) * LANES] = mixed
        lab_k[t * LANES : (t + 1) * LANES] = jnp.broadcast_to(mixed, (LANES, LANES)).T
    acc[...] = jnp.full(acc.shape, -1.0, jnp.float32)

    def best_of(gram, k0, q0, own):
        kn, qn = gram.shape
        same = jnp.concatenate([lab_k[pl.ds(k0, kn)]] * (qn // LANES), axis=1) == lab_q[:, q0 : q0 + qn]
        if own:
            same = same & (iota((kn, qn), 0) + k0 != iota((kn, qn), 1) + q0)
        return jnp.where(same, gram, -1.0)

    def meet(k0, kn, q0, qn, own):
        best = best_of(product(keys[pl.ds(k0, kn)], keys[q0 : q0 + qn], NT), k0, q0, own)
        acc[:, q0 : q0 + qn] = jnp.maximum(acc[:, q0 : q0 + qn], jnp.max(best.reshape(kn // 8, 8, qn), axis=0))
        return best

    def meet_all(k0, kn, q0, qn, own):
        size = math.gcd(kn, 2 * LANES)

        @pl.loop(0, kn // size)
        def _(i):
            meet(pl.multiple_of(k0 + i * size, LANES), size, q0, qn, own)

    def rows_of(g, ref):
        low, high = GROUPS[g]
        low = max(low, 1)
        return ref.at[pl.ds(low * block, (high - low) * block)]

    for g in range(LAST):
        all_of(rows_of(g, keys), data_rs.at[g])
        forward_copy(g).start()
        forward_copy(g).wait_recv()
        low, high = GROUPS[g]
        old, new, end = low * block, (high - low) * block, high * block
        meet_all(old, new, 0, end, True)
        meet_all(items + old, new, 0, end, False)
        if old:
            meet_all(0, old, old, new, False)
            meet_all(items, old, old, new, False)
    old = GROUPS[LAST][0] * block
    new = items - old
    for g in range(LAST, len(GROUPS)):
        all_of(rows_of(g, keys), data_rs.at[g])
        forward_copy(g).start()
    here = meet(old, new, 0, items, True)
    there = best_of(product(keys[old:items], keys[items : items + old], NT), old, items, False)
    column = jnp.maximum(jnp.max(here, axis=1, keepdims=True), jnp.max(there, axis=1, keepdims=True))
    line = jnp.broadcast_to(column, (new, LANES)).T[:8]
    acc[:, old:] = jnp.maximum(acc[:, old:], line)
    for g in range(LAST, len(GROUPS)):
        forward_copy(g).wait_recv()
    meet(items + old, new, 0, items, False)

    best = jnp.max(acc[...], axis=0, keepdims=True)
    kinds = 8
    kind = iota((kinds, items), 0).astype(jnp.float32)
    mine = jnp.where(kind == lab_q[:, :items], 1.0, 0.0)
    other = jnp.where(kind == lab_q[:, items:], 1.0, 0.0)
    numbers = jnp.sum(mine + other, axis=1, keepdims=True)
    part = jnp.sum(mine * best, axis=1, keepdims=True) / jnp.maximum(numbers, 1.0)
    spread = jnp.where(iota((kinds, LANES), 0) == lax.rem(iota((kinds, LANES), 1), kinds), part, 0.0)
    parts = jnp.sum(spread, axis=0, keepdims=True)
    par_s[...] = parts
    for pos in range(chips):
        first = pos // per * LANES
        packed = jnp.where(quarter == pos % per, best[:, first : first + LANES], parts)
        if pos == 0:
            ret_r[0] = packed
        else:
            ret_s[pos] = packed
    for pos in sorted(range(chips), key=lambda pos: -abs(ahead[pos])):
        if pos > 0:
            return_copy(pos).start()
        part_copy(pos).start()
    all_of(send.at[pl.ds(block, items - block)], data_ss)
    all_of(keys.at[pl.ds(0, items)], fwd_ss)
    all_of(lab_r.at[pl.ds(1, chips - 1)], lab_ss)
    labels_over.wait_send()
    total = items + clusters
    here = jnp.where(iota((chips, total), 0) == place[...], 1.0, 0.0).astype(jnp.bfloat16)
    here = jnp.concatenate([here] * 3, axis=0)
    wanted = iota((LANES, total), 0) == lane_at[...]
    all_of(ret_r.at[pl.ds(1, chips - 1)], ret_rs)
    all_of(par_r, par_rs)

    def looked_up(rows, low, high):
        rows = jnp.concatenate(three_parts(jnp.concatenate(rows, axis=0)), axis=0)
        values = product(rows, here[:, low:high], TN)
        return jnp.sum(jnp.where(wanted[:, low:high], values, 0.0), axis=0, keepdims=True)

    out_ref[:, items:] = looked_up([ret_r[pos] + par_r[pos] for pos in range(chips)], items, total)
    out_ref[:, :items] = looked_up([ret_r[pos] for pos in range(chips)], 0, items)
    store = pltpu.make_async_copy(out_ref, out_hbm, own_sem.at[0])
    store.start()
    all_of(ret_r.at[pl.ds(1, chips - 1)], ret_ss)
    all_of(par_r, par_ss)
    store.wait()


def split(out_hbm, max_hbm, mean_hbm, sem):
    items = max_hbm.shape[1]
    copies = [
        pltpu.make_async_copy(out_hbm.at[:, pl.ds(0, items)], max_hbm, sem.at[0]),
        pltpu.make_async_copy(out_hbm.at[:, pl.ds(items, mean_hbm.shape[1])], mean_hbm, sem.at[1]),
    ]
    for copy in copies:
        copy.start()
    for copy in copies:
        copy.wait()


def body(embeddings, cluster_ids, owner_map):
    chips = lax.axis_size("owner") // 2
    items, width = embeddings.shape
    clusters = owner_map.shape[0]
    anywhere = pl.BlockSpec(memory_space=pl.ANY)
    row = (1, LANES)
    dma = pltpu.SemaphoreType.DMA
    both = pl.pallas_call(
        functools.partial(kernel, chips),
        out_shape=jax.ShapeDtypeStruct((1, items + clusters), jnp.float32),
        in_specs=[anywhere] * 3,
        out_specs=anywhere,
        scratch_shapes=[
            pltpu.VMEM((1, items), jnp.int32),
            pltpu.VMEM((1, clusters), jnp.int32),
            pltpu.VMEM((items, width), jnp.bfloat16),
            pltpu.VMEM((1, items + clusters), jnp.float32),
            pltpu.VMEM((items, width), jnp.bfloat16),
            pltpu.VMEM((2 * items, width), jnp.bfloat16),
            pltpu.VMEM((items // LANES, *row), jnp.float32),
            pltpu.VMEM((2 * chips, *row), jnp.float32),
            pltpu.VMEM((1, 2 * items), jnp.float32),
            pltpu.VMEM((2 * items, LANES), jnp.float32),
            pltpu.VMEM((8, items), jnp.float32),
            pltpu.VMEM((chips, *row), jnp.float32),
            pltpu.VMEM((chips, *row), jnp.float32),
            pltpu.VMEM(row, jnp.float32),
            pltpu.VMEM((chips, *row), jnp.float32),
            pltpu.VMEM((1, items + clusters), jnp.int32),
            pltpu.VMEM((1, items + clusters), jnp.int32),
            dma, dma((len(GROUPS),)), dma, dma, dma, dma((len(GROUPS),)),
            dma, dma, dma, dma, dma, dma, dma((3,)),
            pltpu.SemaphoreType.REGULAR((4,)),
        ],
        compiler_params=pltpu.CompilerParams(collective_id=0, has_side_effects=True),
    )(cluster_ids.reshape(1, items), owner_map.reshape(1, clusters), embeddings)
    maxima, means = pl.pallas_call(
        split,
        out_shape=(
            jax.ShapeDtypeStruct((1, items), jnp.float32),
            jax.ShapeDtypeStruct((1, clusters), jnp.float32),
        ),
        in_specs=[anywhere],
        out_specs=(anywhere, anywhere),
        scratch_shapes=[dma((2,))],
    )(both)
    return maxima.reshape(items), means.reshape(clusters)


def solution(mesh):
    placed = (P(("parts", "owner"), None), P(("parts", "owner")), P("parts"))
    return jax.shard_map(
        body,
        mesh=mesh,
        in_specs=placed,
        out_specs=(P(("parts", "owner")), P("parts")),
        check_vma=False,
    )
```

```python
import functools
import math

import jax
import jax.numpy as jnp
from jax import lax
from jax.experimental import pallas as pl
from jax.experimental.pallas import tpu as pltpu
from jax.sharding import PartitionSpec as P

MESH = pl.DeviceIdType.MESH
LANES = 128
GROUPS = ((0, 16), (16, 24), (24, 28), (28, 32))
LAST = 2
NT = (((1,), (1,)), ((), ()))
TN = (((0,), (0,)), ((), ()))


def iota(shape, dim):
    return lax.broadcasted_iota(jnp.int32, shape, dim)


def upto(n):
    return jnp.where(iota((n, n), 0) <= iota((n, n), 1), 1.0, 0.0).astype(jnp.bfloat16)


def product(a, b, dims=(((1,), (0,)), ((), ()))):
    return lax.dot_general(a, b, dims, preferred_element_type=jnp.float32)


def deltas(chips):
    half, near = chips // 2, (2, 3, 4, 5)
    order = [0, *(d * way for d in near for way in (1, -1)), half]
    far = [d for d in range(half - 1, 0, -1) if d not in near]
    return order + [d * way for d in far for way in (1, -1)]


def place_of(ahead, chips):
    place = jnp.zeros_like(ahead)
    for pos, delta in enumerate(deltas(chips)):
        place = jnp.where(ahead == delta % chips, pos, place)
    return place


def three_parts(x):
    high = x.astype(jnp.bfloat16)
    rest = x - high.astype(jnp.float32)
    middle = rest.astype(jnp.bfloat16)
    low = (rest - middle.astype(jnp.float32)).astype(jnp.bfloat16)
    return high, middle, low


def kernel(
    chips, ids_hbm, map_hbm, rows_hbm, out_hbm,
    ids_ref, map_ref, rows_ref, out_ref, send, keys, lab_s, lab_r, lab_q, lab_k, acc, ret_s, ret_r, par_s, par_r, place, lane_at,
    data_ss, data_rs, lab_ss, lab_rs, fwd_ss, fwd_rs, ret_ss, ret_rs, par_ss, par_rs, two_ss, two_rs, own_sem, known,
):
    items, width = rows_ref.shape
    clusters = map_ref.shape[1]
    block = items // chips
    per = LANES // block
    me = lax.axis_index("owner")
    core, z = lax.rem(me, 2), me // 2
    partner = {"owner": z * 2 + 1 - core}

    def chip(delta, which=core):
        return {"owner": lax.rem(z + delta + 2 * chips, chips) * 2 + which}

    def all_of(ref, semaphore):
        pltpu.make_async_copy(ref, ref, semaphore).wait()

    def signal(semaphore, device):
        pl.semaphore_signal(semaphore, inc=1, device_id=device, device_id_type=MESH)

    ahead = deltas(chips)
    barrier = pltpu.get_barrier_semaphore()
    for device in (chip(1), chip(-1), partner):
        signal(barrier, device)
    loads = [
        pltpu.make_async_copy(source, target, own_sem.at[i])
        for i, (source, target) in enumerate(((ids_hbm, ids_ref), (map_hbm, map_ref), (rows_hbm, rows_ref)))
    ]
    for load in loads:
        load.start()

    levels = math.ceil(math.log2(chips // 2))

    def tell(level):
        for way in (1, -1):
            signal(known.at[level], chip(way * 2**level))

    def learn(level):
        pl.semaphore_wait(known.at[level], 2)

    pl.semaphore_wait(barrier, 3)
    tell(0)
    loads[0].wait()
    loads[1].wait()

    pair_c = lax.shift_right_logical(map_ref[...], 1)
    place_c = place_of(lax.rem(pair_c - z + chips, chips), chips)
    at_c = jnp.where(iota((chips, clusters), 0) == place_c, 1.0, 0.0)
    count_c = product(at_c.astype(jnp.bfloat16), upto(clusters))
    local_c = jnp.sum(at_c * count_c, axis=0, keepdims=True) - 1.0

    hits = jnp.where(iota((clusters, items), 0) == ids_ref[...], 1.0, 0.0).astype(jnp.bfloat16)
    table = jnp.concatenate([at_c, jnp.broadcast_to(local_c, (16, clusters))], axis=0).astype(jnp.bfloat16)
    found = product(table, hits)
    at = found[:chips]
    label = found[chips:].astype(jnp.bfloat16)
    tiles = items // LANES
    stacked = jnp.concatenate([at[:, t * LANES : (t + 1) * LANES] for t in range(tiles)], axis=0)
    sums = product(stacked.astype(jnp.bfloat16), upto(LANES))
    row = iota((chips, LANES), 0).astype(jnp.float32)
    before = jnp.zeros((chips, 1), jnp.float32)
    places, slots = [], []
    for t in range(tiles):
        at_t = stacked[t * chips : (t + 1) * chips]
        sum_t = sums[t * chips : (t + 1) * chips]
        places.append(jnp.sum(at_t * row, axis=0, keepdims=True))
        slots.append(jnp.sum(at_t * (sum_t + before + row * block), axis=0, keepdims=True) - 1.0)
        before = before + sum_t[:, LANES - 1 :]
    place_i = jnp.concatenate(places, axis=1).astype(jnp.int32)
    slot = jnp.concatenate(slots, axis=1).astype(jnp.int32)
    place[:, :items] = place_i
    place[:, items:] = place_c
    lane_at[:, :items] = lax.rem(slot, LANES)
    lane_at[:, items:] = lax.rem(place_c + 1, per) * block + local_c.astype(jnp.int32)

    group_of = {pos: g for g, (low, high) in enumerate(GROUPS) for pos in range(low, high)}

    def data_copy(pos):
        return pltpu.make_async_remote_copy(
            src_ref=send.at[pl.ds(pos * block, block)], dst_ref=keys.at[pl.ds(pos * block, block)],
            send_sem=data_ss, recv_sem=data_rs.at[group_of[pos]],
            device_id=chip(ahead[pos]), device_id_type=MESH,
        )

    def label_copy(pos):
        return pltpu.make_async_remote_copy(
            src_ref=lab_s.at[pos // per], dst_ref=lab_r.at[pos],
            send_sem=lab_ss, recv_sem=lab_rs,
            device_id=chip(ahead[pos]), device_id_type=MESH,
        )

    def forward_copy(g):
        low, high = GROUPS[g]
        return pltpu.make_async_remote_copy(
            src_ref=keys.at[pl.ds(low * block, (high - low) * block)],
            dst_ref=keys.at[pl.ds(items + low * block, (high - low) * block)],
            send_sem=fwd_ss, recv_sem=fwd_rs.at[g], device_id=partner, device_id_type=MESH,
        )

    def return_copy(pos):
        return pltpu.make_async_remote_copy(
            src_ref=ret_s.at[pos], dst_ref=ret_r.at[pos],
            send_sem=ret_ss, recv_sem=ret_rs,
            device_id=chip(-ahead[pos]), device_id_type=MESH,
        )

    def part_copy(pos):
        return pltpu.make_async_remote_copy(
            src_ref=par_s, dst_ref=par_r.at[pos],
            send_sem=par_ss, recv_sem=par_rs,
            device_id=chip(-ahead[pos], 1 - core), device_id_type=MESH,
        )

    labels_over = pltpu.make_async_remote_copy(
        src_ref=lab_r.at[pl.ds(0, chips)], dst_ref=lab_r.at[pl.ds(chips, chips)],
        send_sem=two_ss, recv_sem=two_rs, device_id=partner, device_id_type=MESH,
    )

    step = 2 * LANES

    def arrange(first):
        pick = jnp.where(iota((step, items), 0) + first == slot, 1.0, 0.0).astype(jnp.bfloat16)
        rows = product(pick, rows_ref[...])
        scale = lax.rsqrt(jnp.mean(rows * rows, axis=1, keepdims=True) + 1e-06)
        unit = (rows * scale * jnp.float32(width**-0.5)).astype(jnp.bfloat16)
        send[first : first + step] = unit
        names = product(label, pick, NT)
        for t in range(step // LANES):
            lab_s[first // LANES + t] = names[:1, t * LANES : (t + 1) * LANES]
        if first == 0:
            keys[:block] = unit[:block]
            lab_r[0] = names[:1, :LANES]

    def start(copy, low, high):
        for pos in range(1, chips):
            if low <= abs(ahead[pos]) <= high:
                copy(pos).start()

    loads[2].wait()
    arrange(0)
    learn(0)
    tell(1)
    start(data_copy, 2, 2)
    start(label_copy, 2, 2)
    arrange(step)
    learn(1)
    tell(2)
    start(data_copy, 3, 4)
    start(label_copy, 3, 4)
    for first in range(2 * step, items, step):
        arrange(first)
    start(label_copy, 1, 1)
    for level in range(2, levels):
        learn(level)
        if level + 1 < levels:
            tell(level + 1)
        start(label_copy, 2**level + 1, 2 ** (level + 1))
        if level == 2:
            start(data_copy, 5, 5)
    start(data_copy, 6, chips)
    start(data_copy, 1, 1)

    all_of(lab_r.at[pl.ds(1, chips - 1)], lab_rs)
    labels_over.start()
    labels_over.wait_recv()
    quarter = lax.div(iota((1, LANES), 1), block)
    for t in range(2 * tiles):
        mixed = jnp.zeros((1, LANES), jnp.float32)
        for q in range(per):
            mixed = jnp.where(quarter == q, lab_r[t * per + q], mixed)
        lab_q[:, t * LANES : (t + 1) * LANES] = mixed
        lab_k[t * LANES : (t + 1) * LANES] = jnp.broadcast_to(mixed, (LANES, LANES)).T
    acc[...] = jnp.full(acc.shape, -1.0, jnp.float32)

    def best_of(gram, k0, q0, own):
        kn, qn = gram.shape
        same = jnp.concatenate([lab_k[pl.ds(k0, kn)]] * (qn // LANES), axis=1) == lab_q[:, q0 : q0 + qn]
        if own:
            same = same & (iota((kn, qn), 0) + k0 != iota((kn, qn), 1) + q0)
        return jnp.where(same, gram, -1.0)

    def meet(k0, kn, q0, qn, own):
        best = best_of(product(keys[pl.ds(k0, kn)], keys[q0 : q0 + qn], NT), k0, q0, own)
        acc[:, q0 : q0 + qn] = jnp.maximum(acc[:, q0 : q0 + qn], jnp.max(best.reshape(kn // 8, 8, qn), axis=0))
        return best

    def meet_all(k0, kn, q0, qn, own):
        size = math.gcd(kn, 2 * LANES)

        @pl.loop(0, kn // size)
        def _(i):
            meet(pl.multiple_of(k0 + i * size, LANES), size, q0, qn, own)

    def rows_of(g, ref):
        low, high = GROUPS[g]
        low = max(low, 1)
        return ref.at[pl.ds(low * block, (high - low) * block)]

    for g in range(LAST):
        all_of(rows_of(g, keys), data_rs.at[g])
        forward_copy(g).start()
        forward_copy(g).wait_recv()
        low, high = GROUPS[g]
        old, new, end = low * block, (high - low) * block, high * block
        meet_all(old, new, 0, end, True)
        meet_all(items + old, new, 0, end, False)
        if old:
            meet_all(0, old, old, new, False)
            meet_all(items, old, old, new, False)
    old = GROUPS[LAST][0] * block
    new = items - old
    for g in range(LAST, len(GROUPS)):
        all_of(rows_of(g, keys), data_rs.at[g])
        forward_copy(g).start()
    here = meet(old, new, 0, items, True)
    there = best_of(product(keys[old:items], keys[items : items + old], NT), old, items, False)
    column = jnp.maximum(jnp.max(here, axis=1, keepdims=True), jnp.max(there, axis=1, keepdims=True))
    line = jnp.broadcast_to(column, (new, LANES)).T[:8]
    acc[:, old:] = jnp.maximum(acc[:, old:], line)
    for g in range(LAST, len(GROUPS)):
        forward_copy(g).wait_recv()
    meet(items + old, new, 0, items, False)

    best = jnp.max(acc[...], axis=0, keepdims=True)
    kinds = 8
    kind = iota((kinds, items), 0).astype(jnp.float32)
    mine = jnp.where(kind == lab_q[:, :items], 1.0, 0.0)
    other = jnp.where(kind == lab_q[:, items:], 1.0, 0.0)
    numbers = jnp.sum(mine + other, axis=1, keepdims=True)
    part = jnp.sum(mine * best, axis=1, keepdims=True) / jnp.maximum(numbers, 1.0)
    spread = jnp.where(iota((kinds, LANES), 0) == lax.rem(iota((kinds, LANES), 1), kinds), part, 0.0)
    parts = jnp.sum(spread, axis=0, keepdims=True)
    par_s[...] = parts
    for pos in range(chips):
        first = pos // per * LANES
        packed = jnp.where(quarter == pos % per, best[:, first : first + LANES], parts)
        if pos == 0:
            ret_r[0] = packed
        else:
            ret_s[pos] = packed
    for pos in sorted(range(chips), key=lambda pos: -abs(ahead[pos])):
        if pos > 0:
            return_copy(pos).start()
        part_copy(pos).start()
    all_of(send.at[pl.ds(block, items - block)], data_ss)
    all_of(keys.at[pl.ds(0, items)], fwd_ss)
    all_of(lab_r.at[pl.ds(1, chips - 1)], lab_ss)
    labels_over.wait_send()
    total = items + clusters
    here = jnp.where(iota((chips, total), 0) == place[...], 1.0, 0.0).astype(jnp.bfloat16)
    here = jnp.concatenate([here] * 3, axis=0)
    wanted = iota((LANES, total), 0) == lane_at[...]
    all_of(ret_r.at[pl.ds(1, chips - 1)], ret_rs)
    all_of(par_r, par_rs)

    def looked_up(rows, low, high):
        rows = jnp.concatenate(three_parts(jnp.concatenate(rows, axis=0)), axis=0)
        values = product(rows, here[:, low:high], TN)
        return jnp.sum(jnp.where(wanted[:, low:high], values, 0.0), axis=0, keepdims=True)

    out_ref[:, items:] = looked_up([ret_r[pos] + par_r[pos] for pos in range(chips)], items, total)
    out_ref[:, :items] = looked_up([ret_r[pos] for pos in range(chips)], 0, items)
    store = pltpu.make_async_copy(out_ref, out_hbm, own_sem.at[0])
    store.start()
    all_of(ret_r.at[pl.ds(1, chips - 1)], ret_ss)
    all_of(par_r, par_ss)
    store.wait()


def split(out_hbm, max_hbm, mean_hbm, sem):
    items = max_hbm.shape[1]
    copies = [
        pltpu.make_async_copy(out_hbm.at[:, pl.ds(0, items)], max_hbm, sem.at[0]),
        pltpu.make_async_copy(out_hbm.at[:, pl.ds(items, mean_hbm.shape[1])], mean_hbm, sem.at[1]),
    ]
    for copy in copies:
        copy.start()
    for copy in copies:
        copy.wait()


def body(embeddings, cluster_ids, owner_map):
    chips = lax.axis_size("owner") // 2
    items, width = embeddings.shape
    clusters = owner_map.shape[0]
    anywhere = pl.BlockSpec(memory_space=pl.ANY)
    row = (1, LANES)
    dma = pltpu.SemaphoreType.DMA
    both = pl.pallas_call(
        functools.partial(kernel, chips),
        out_shape=jax.ShapeDtypeStruct((1, items + clusters), jnp.float32),
        in_specs=[anywhere] * 3,
        out_specs=anywhere,
        scratch_shapes=[
            pltpu.VMEM((1, items), jnp.int32),
            pltpu.VMEM((1, clusters), jnp.int32),
            pltpu.VMEM((items, width), jnp.bfloat16),
            pltpu.VMEM((1, items + clusters), jnp.float32),
            pltpu.VMEM((items, width), jnp.bfloat16),
            pltpu.VMEM((2 * items, width), jnp.bfloat16),
            pltpu.VMEM((items // LANES, *row), jnp.float32),
            pltpu.VMEM((2 * chips, *row), jnp.float32),
            pltpu.VMEM((1, 2 * items), jnp.float32),
            pltpu.VMEM((2 * items, LANES), jnp.float32),
            pltpu.VMEM((8, items), jnp.float32),
            pltpu.VMEM((chips, *row), jnp.float32),
            pltpu.VMEM((chips, *row), jnp.float32),
            pltpu.VMEM(row, jnp.float32),
            pltpu.VMEM((chips, *row), jnp.float32),
            pltpu.VMEM((1, items + clusters), jnp.int32),
            pltpu.VMEM((1, items + clusters), jnp.int32),
            dma, dma((len(GROUPS),)), dma, dma, dma, dma((len(GROUPS),)),
            dma, dma, dma, dma, dma, dma, dma((3,)),
            pltpu.SemaphoreType.REGULAR((4,)),
        ],
        compiler_params=pltpu.CompilerParams(collective_id=0, has_side_effects=True, vmem_limit_bytes=32 * 2**20),
    )(*[
        pltpu.with_memory_space_constraint(array, pltpu.HBM)
        for array in (cluster_ids.reshape(1, items), owner_map.reshape(1, clusters), embeddings)
    ])
    maxima, means = pl.pallas_call(
        split,
        out_shape=(
            jax.ShapeDtypeStruct((1, items), jnp.float32),
            jax.ShapeDtypeStruct((1, clusters), jnp.float32),
        ),
        in_specs=[anywhere],
        out_specs=(anywhere, anywhere),
        scratch_shapes=[dma((2,))],
        compiler_params=pltpu.CompilerParams(vmem_limit_bytes=2**20),
    )(both)
    return maxima.reshape(items), means.reshape(clusters)


def solution(mesh):
    placed = (P(("parts", "owner"), None), P(("parts", "owner")), P("parts"))
    return jax.shard_map(
        body,
        mesh=mesh,
        in_specs=placed,
        out_specs=(P(("parts", "owner")), P("parts")),
        check_vma=False,
    )
```

```python
import functools
import math

import jax
import jax.numpy as jnp
from jax import lax
from jax.experimental import pallas as pl
from jax.experimental.pallas import tpu as pltpu
from jax.sharding import PartitionSpec as P

MESH = pl.DeviceIdType.MESH
LANES = 128
GROUPS = ((0, 16), (16, 24), (24, 28), (28, 32))
LAST = 2
NT = (((1,), (1,)), ((), ()))
TN = (((0,), (0,)), ((), ()))


def iota(shape, dim):
    return lax.broadcasted_iota(jnp.int32, shape, dim)


def upto(n):
    return jnp.where(iota((n, n), 0) <= iota((n, n), 1), 1.0, 0.0).astype(jnp.bfloat16)


def product(a, b, dims=(((1,), (0,)), ((), ()))):
    return lax.dot_general(a, b, dims, preferred_element_type=jnp.float32)


def deltas(chips):
    half, near = chips // 2, (2, 3, 4, 5)
    order = [0, *(d * way for d in near for way in (1, -1)), half]
    far = [d for d in range(half - 1, 0, -1) if d not in near]
    return order + [d * way for d in far for way in (1, -1)]


def place_of(ahead, chips):
    place = jnp.zeros_like(ahead)
    for pos, delta in enumerate(deltas(chips)):
        place = jnp.where(ahead == delta % chips, pos, place)
    return place


def three_parts(x):
    high = x.astype(jnp.bfloat16)
    rest = x - high.astype(jnp.float32)
    middle = rest.astype(jnp.bfloat16)
    low = (rest - middle.astype(jnp.float32)).astype(jnp.bfloat16)
    return high, middle, low


def kernel(
    chips, ids_hbm, map_hbm, rows_hbm, out_hbm,
    ids_ref, map_ref, rows_ref, out_ref, send, keys, lab_s, lab_r, lab_q, lab_k, acc, ret_s, ret_r, par_s, par_r, place, lane_at,
    data_ss, data_rs, lab_ss, lab_rs, fwd_ss, fwd_rs, ret_ss, ret_rs, par_ss, par_rs, two_ss, two_rs, own_sem, known,
):
    items, width = rows_ref.shape
    clusters = map_ref.shape[1]
    block = items // chips
    per = LANES // block
    me = lax.axis_index("owner")
    core, z = lax.rem(me, 2), me // 2
    partner = {"owner": z * 2 + 1 - core}

    def chip(delta, which=core):
        return {"owner": lax.rem(z + delta + 2 * chips, chips) * 2 + which}

    def all_of(ref, semaphore):
        pltpu.make_async_copy(ref, ref, semaphore).wait()

    def signal(semaphore, device):
        pl.semaphore_signal(semaphore, inc=1, device_id=device, device_id_type=MESH)

    ahead = deltas(chips)
    barrier = pltpu.get_barrier_semaphore()
    for device in (chip(1), chip(-1), partner):
        signal(barrier, device)
    loads = [
        pltpu.make_async_copy(source, target, own_sem.at[i])
        for i, (source, target) in enumerate(((ids_hbm, ids_ref), (map_hbm, map_ref), (rows_hbm, rows_ref)))
    ]
    for load in loads:
        load.start()

    levels = math.ceil(math.log2(chips // 2))

    def tell(level):
        for way in (1, -1):
            signal(known.at[level], chip(way * 2**level))

    def learn(level):
        pl.semaphore_wait(known.at[level], 2)

    pl.semaphore_wait(barrier, 3)
    tell(0)
    loads[0].wait()
    loads[1].wait()

    pair_c = lax.shift_right_logical(map_ref[...], 1)
    place_c = place_of(lax.rem(pair_c - z + chips, chips), chips)
    at_c = jnp.where(iota((chips, clusters), 0) == place_c, 1.0, 0.0)
    count_c = product(at_c.astype(jnp.bfloat16), upto(clusters))
    local_c = jnp.sum(at_c * count_c, axis=0, keepdims=True) - 1.0

    hits = jnp.where(iota((clusters, items), 0) == ids_ref[...], 1.0, 0.0).astype(jnp.bfloat16)
    table = jnp.concatenate([at_c, jnp.broadcast_to(local_c, (16, clusters))], axis=0).astype(jnp.bfloat16)
    found = product(table, hits)
    at = found[:chips]
    label = found[chips:].astype(jnp.bfloat16)
    tiles = items // LANES
    stacked = jnp.concatenate([at[:, t * LANES : (t + 1) * LANES] for t in range(tiles)], axis=0)
    sums = product(stacked.astype(jnp.bfloat16), upto(LANES))
    row = iota((chips, LANES), 0).astype(jnp.float32)
    before = jnp.zeros((chips, 1), jnp.float32)
    places, slots = [], []
    for t in range(tiles):
        at_t = stacked[t * chips : (t + 1) * chips]
        sum_t = sums[t * chips : (t + 1) * chips]
        places.append(jnp.sum(at_t * row, axis=0, keepdims=True))
        slots.append(jnp.sum(at_t * (sum_t + before + row * block), axis=0, keepdims=True) - 1.0)
        before = before + sum_t[:, LANES - 1 :]
    place_i = jnp.concatenate(places, axis=1).astype(jnp.int32)
    slot = jnp.concatenate(slots, axis=1).astype(jnp.int32)
    place[:, :items] = place_i
    place[:, items:] = place_c
    lane_at[:, :items] = lax.rem(slot, LANES)
    lane_at[:, items:] = lax.rem(place_c + 1, per) * block + local_c.astype(jnp.int32)

    group_of = {pos: g for g, (low, high) in enumerate(GROUPS) for pos in range(low, high)}

    def data_copy(pos):
        return pltpu.make_async_remote_copy(
            src_ref=send.at[pl.ds(pos * block, block)], dst_ref=keys.at[pl.ds(pos * block, block)],
            send_sem=data_ss, recv_sem=data_rs.at[group_of[pos]],
            device_id=chip(ahead[pos]), device_id_type=MESH,
        )

    def label_copy(pos):
        return pltpu.make_async_remote_copy(
            src_ref=lab_s.at[pos // per], dst_ref=lab_r.at[pos],
            send_sem=lab_ss, recv_sem=lab_rs,
            device_id=chip(ahead[pos]), device_id_type=MESH,
        )

    def forward_copy(g):
        low, high = GROUPS[g]
        return pltpu.make_async_remote_copy(
            src_ref=keys.at[pl.ds(low * block, (high - low) * block)],
            dst_ref=keys.at[pl.ds(items + low * block, (high - low) * block)],
            send_sem=fwd_ss, recv_sem=fwd_rs.at[g], device_id=partner, device_id_type=MESH,
        )

    def return_copy(pos):
        return pltpu.make_async_remote_copy(
            src_ref=ret_s.at[pos], dst_ref=ret_r.at[pos],
            send_sem=ret_ss, recv_sem=ret_rs,
            device_id=chip(-ahead[pos]), device_id_type=MESH,
        )

    def part_copy(pos):
        return pltpu.make_async_remote_copy(
            src_ref=par_s, dst_ref=par_r.at[pos],
            send_sem=par_ss, recv_sem=par_rs,
            device_id=chip(-ahead[pos], 1 - core), device_id_type=MESH,
        )

    labels_over = pltpu.make_async_remote_copy(
        src_ref=lab_r.at[pl.ds(0, chips)], dst_ref=lab_r.at[pl.ds(chips, chips)],
        send_sem=two_ss, recv_sem=two_rs, device_id=partner, device_id_type=MESH,
    )

    step = 2 * LANES

    def arrange(first):
        pick = jnp.where(iota((step, items), 0) + first == slot, 1.0, 0.0).astype(jnp.bfloat16)
        rows = product(pick, rows_ref[...])
        scale = lax.rsqrt(jnp.mean(rows * rows, axis=1, keepdims=True) + 1e-06)
        unit = (rows * scale * jnp.float32(width**-0.5)).astype(jnp.bfloat16)
        send[first : first + step] = unit
        names = product(label, pick, NT)
        for t in range(step // LANES):
            lab_s[first // LANES + t] = names[:1, t * LANES : (t + 1) * LANES]
        if first == 0:
            keys[:block] = unit[:block]
            lab_r[0] = names[:1, :LANES]

    def start(copy, low, high):
        for pos in range(1, chips):
            if low <= abs(ahead[pos]) <= high:
                copy(pos).start()

    loads[2].wait()
    arrange(0)
    learn(0)
    tell(1)
    start(data_copy, 2, 2)
    start(label_copy, 2, 2)
    arrange(step)
    learn(1)
    tell(2)
    start(data_copy, 3, 4)
    start(label_copy, 3, 4)
    for first in range(2 * step, items, step):
        arrange(first)
    for level in range(2, levels):
        learn(level)
        if level + 1 < levels:
            tell(level + 1)
        start(label_copy, 2**level + 1, 2 ** (level + 1))
        if level == 2:
            start(label_copy, 1, 1)
            start(data_copy, 5, 5)
    start(data_copy, 6, chips)
    start(data_copy, 1, 1)

    all_of(lab_r.at[pl.ds(1, chips - 1)], lab_rs)
    labels_over.start()
    labels_over.wait_recv()
    quarter = lax.div(iota((1, LANES), 1), block)
    for t in range(2 * tiles):
        mixed = jnp.zeros((1, LANES), jnp.float32)
        for q in range(per):
            mixed = jnp.where(quarter == q, lab_r[t * per + q], mixed)
        lab_q[:, t * LANES : (t + 1) * LANES] = mixed
        lab_k[t * LANES : (t + 1) * LANES] = jnp.broadcast_to(mixed, (LANES, LANES)).T
    acc[...] = jnp.full(acc.shape, -1.0, jnp.float32)

    def best_of(gram, k0, q0, own):
        kn, qn = gram.shape
        same = jnp.concatenate([lab_k[pl.ds(k0, kn)]] * (qn // LANES), axis=1) == lab_q[:, q0 : q0 + qn]
        if own:
            same = same & (iota((kn, qn), 0) + k0 != iota((kn, qn), 1) + q0)
        return jnp.where(same, gram, -1.0)

    def meet(k0, kn, q0, qn, own):
        best = best_of(product(keys[pl.ds(k0, kn)], keys[q0 : q0 + qn], NT), k0, q0, own)
        acc[:, q0 : q0 + qn] = jnp.maximum(acc[:, q0 : q0 + qn], jnp.max(best.reshape(kn // 8, 8, qn), axis=0))
        return best

    def meet_all(k0, kn, q0, qn, own):
        size = math.gcd(kn, 2 * LANES)

        @pl.loop(0, kn // size)
        def _(i):
            meet(pl.multiple_of(k0 + i * size, LANES), size, q0, qn, own)

    def rows_of(g, ref):
        low, high = GROUPS[g]
        low = max(low, 1)
        return ref.at[pl.ds(low * block, (high - low) * block)]

    for g in range(LAST):
        all_of(rows_of(g, keys), data_rs.at[g])
        forward_copy(g).start()
        forward_copy(g).wait_recv()
        low, high = GROUPS[g]
        old, new, end = low * block, (high - low) * block, high * block
        meet_all(old, new, 0, end, True)
        meet_all(items + old, new, 0, end, False)
        if old:
            meet_all(0, old, old, new, False)
            meet_all(items, old, old, new, False)
    old = GROUPS[LAST][0] * block
    new = items - old
    for g in range(LAST, len(GROUPS)):
        all_of(rows_of(g, keys), data_rs.at[g])
        forward_copy(g).start()
    here = meet(old, new, 0, items, True)
    there = best_of(product(keys[old:items], keys[items : items + old], NT), old, items, False)
    column = jnp.maximum(jnp.max(here, axis=1, keepdims=True), jnp.max(there, axis=1, keepdims=True))
    line = jnp.broadcast_to(column, (new, LANES)).T[:8]
    acc[:, old:] = jnp.maximum(acc[:, old:], line)
    for g in range(LAST, len(GROUPS)):
        forward_copy(g).wait_recv()
    meet(items + old, new, 0, items, False)

    best = jnp.max(acc[...], axis=0, keepdims=True)
    kinds = 8
    kind = iota((kinds, items), 0).astype(jnp.float32)
    mine = jnp.where(kind == lab_q[:, :items], 1.0, 0.0)
    other = jnp.where(kind == lab_q[:, items:], 1.0, 0.0)
    numbers = jnp.sum(mine + other, axis=1, keepdims=True)
    part = jnp.sum(mine * best, axis=1, keepdims=True) / jnp.maximum(numbers, 1.0)
    spread = jnp.where(iota((kinds, LANES), 0) == lax.rem(iota((kinds, LANES), 1), kinds), part, 0.0)
    parts = jnp.sum(spread, axis=0, keepdims=True)
    par_s[...] = parts
    for pos in range(chips):
        first = pos // per * LANES
        packed = jnp.where(quarter == pos % per, best[:, first : first + LANES], parts)
        if pos == 0:
            ret_r[0] = packed
        else:
            ret_s[pos] = packed
    for pos in sorted(range(chips), key=lambda pos: -abs(ahead[pos])):
        if pos > 0:
            return_copy(pos).start()
        part_copy(pos).start()
    all_of(send.at[pl.ds(block, items - block)], data_ss)
    all_of(keys.at[pl.ds(0, items)], fwd_ss)
    all_of(lab_r.at[pl.ds(1, chips - 1)], lab_ss)
    labels_over.wait_send()
    total = items + clusters
    here = jnp.where(iota((chips, total), 0) == place[...], 1.0, 0.0).astype(jnp.bfloat16)
    here = jnp.concatenate([here] * 3, axis=0)
    wanted = iota((LANES, total), 0) == lane_at[...]
    all_of(ret_r.at[pl.ds(1, chips - 1)], ret_rs)
    all_of(par_r, par_rs)

    def looked_up(rows, low, high):
        rows = jnp.concatenate(three_parts(jnp.concatenate(rows, axis=0)), axis=0)
        values = product(rows, here[:, low:high], TN)
        return jnp.sum(jnp.where(wanted[:, low:high], values, 0.0), axis=0, keepdims=True)

    out_ref[:, items:] = looked_up([ret_r[pos] + par_r[pos] for pos in range(chips)], items, total)
    out_ref[:, :items] = looked_up([ret_r[pos] for pos in range(chips)], 0, items)
    store = pltpu.make_async_copy(out_ref, out_hbm, own_sem.at[0])
    store.start()
    all_of(ret_r.at[pl.ds(1, chips - 1)], ret_ss)
    all_of(par_r, par_ss)
    store.wait()


def split(out_hbm, max_hbm, mean_hbm, sem):
    items = max_hbm.shape[1]
    copies = [
        pltpu.make_async_copy(out_hbm.at[:, pl.ds(0, items)], max_hbm, sem.at[0]),
        pltpu.make_async_copy(out_hbm.at[:, pl.ds(items, mean_hbm.shape[1])], mean_hbm, sem.at[1]),
    ]
    for copy in copies:
        copy.start()
    for copy in copies:
        copy.wait()


def body(embeddings, cluster_ids, owner_map):
    chips = lax.axis_size("owner") // 2
    items, width = embeddings.shape
    clusters = owner_map.shape[0]
    anywhere = pl.BlockSpec(memory_space=pl.ANY)
    row = (1, LANES)
    dma = pltpu.SemaphoreType.DMA
    both = pl.pallas_call(
        functools.partial(kernel, chips),
        out_shape=jax.ShapeDtypeStruct((1, items + clusters), jnp.float32),
        in_specs=[anywhere] * 3,
        out_specs=anywhere,
        scratch_shapes=[
            pltpu.VMEM((1, items), jnp.int32),
            pltpu.VMEM((1, clusters), jnp.int32),
            pltpu.VMEM((items, width), jnp.bfloat16),
            pltpu.VMEM((1, items + clusters), jnp.float32),
            pltpu.VMEM((items, width), jnp.bfloat16),
            pltpu.VMEM((2 * items, width), jnp.bfloat16),
            pltpu.VMEM((items // LANES, *row), jnp.float32),
            pltpu.VMEM((2 * chips, *row), jnp.float32),
            pltpu.VMEM((1, 2 * items), jnp.float32),
            pltpu.VMEM((2 * items, LANES), jnp.float32),
            pltpu.VMEM((8, items), jnp.float32),
            pltpu.VMEM((chips, *row), jnp.float32),
            pltpu.VMEM((chips, *row), jnp.float32),
            pltpu.VMEM(row, jnp.float32),
            pltpu.VMEM((chips, *row), jnp.float32),
            pltpu.VMEM((1, items + clusters), jnp.int32),
            pltpu.VMEM((1, items + clusters), jnp.int32),
            dma, dma((len(GROUPS),)), dma, dma, dma, dma((len(GROUPS),)),
            dma, dma, dma, dma, dma, dma, dma((3,)),
            pltpu.SemaphoreType.REGULAR((4,)),
        ],
        compiler_params=pltpu.CompilerParams(collective_id=0, has_side_effects=True, vmem_limit_bytes=32 * 2**20),
    )(*[
        pltpu.with_memory_space_constraint(array, pltpu.HBM)
        for array in (cluster_ids.reshape(1, items), owner_map.reshape(1, clusters), embeddings)
    ])
    maxima, means = pl.pallas_call(
        split,
        out_shape=(
            jax.ShapeDtypeStruct((1, items), jnp.float32),
            jax.ShapeDtypeStruct((1, clusters), jnp.float32),
        ),
        in_specs=[anywhere],
        out_specs=(anywhere, anywhere),
        scratch_shapes=[dma((2,))],
        compiler_params=pltpu.CompilerParams(vmem_limit_bytes=2**20),
    )(both)
    return maxima.reshape(items), means.reshape(clusters)


def solution(mesh):
    placed = (P(("parts", "owner"), None), P(("parts", "owner")), P("parts"))
    return jax.shard_map(
        body,
        mesh=mesh,
        in_specs=placed,
        out_specs=(P(("parts", "owner")), P("parts")),
        check_vma=False,
    )
```
